32 devices in a mesh: ep: 8 (over z, y), tp: 4 (over x, core).
Axes of the slice: x: 2, y: 2, z: 4, core: 2. Of those that a mesh axis runs over, the one named last changes fastest.
Arguments:
- tokens: bfloat16 [4096, 2048], P(('ep', 'tp')), may hold values from -6 to 6
- norm_gain: float32 [2048], replicated, may hold values from 0.1 to 1.9
- expert_ids: int32 [4096, 6], P(('ep', 'tp')), may hold values from 0 to 15, as said below
- slot_index: int32 [4096, 6], P(('ep', 'tp')), may hold values from 0 to 63, as said below
- dropped: int32 [4096, 6], P(('ep', 'tp')), may hold values from 0 to 1, as said below
- gates: float32 [4096, 6], P(('ep', 'tp')), may hold values from 0.05 to 0.8
- w_gate: bfloat16 [16, 2048, 704], P('ep', None, 'tp'), may hold values from -0.125 to 0.125
- w_up: bfloat16 [16, 2048, 704], P('ep', None, 'tp'), may hold values from -0.125 to 0.125
- w_down: bfloat16 [16, 2048, 704], P('ep', None, 'tp'), may hold values from -0.21875 to 0.21875
- shared_gate: bfloat16 [2048, 1408], P(None, 'tp'), may hold values from -0.125 to 0.125
- shared_up: bfloat16 [2048, 1408], P(None, 'tp'), may hold values from -0.125 to 0.125
- shared_down: bfloat16 [1408, 2048], replicated, may hold values from -0.15625 to 0.15625
Outputs:
- layer_out: bfloat16 [4096, 2048], P(('ep', 'tp'))
The draws below stay inside these ranges and needn't reach their ends.
Inputs may be any that keep to these rules, and one draw needn't show every extreme that they name: `expert_ids`: each token names 6 different experts; some expert has 64 kept pairs from the tokens of every device. `slot_index`: for a kept pair, its place among the slots of its expert for the tokens of its device (the tokens n with one value of n // 128); the kept pairs of one device and one expert have distinct places; 0 for a dropped pair. `dropped`: 1 for the pairs of a device and an expert beyond the 64 that are kept.
All inputs are finite; a program needn't handle non-finite values.
Results may differ from the reference program's by a relative error of at most 0.0054.
Values may be sent and summed in bfloat16 or wider, within the bound.
A program may use at most 128 MiB of HBM per device.

```python
import math
import jax
import jax.numpy as jnp
from jax import lax

D = 2048
FF = 704
SFF = 1408
TOP = 6
TOK_DEV = 128
SPECIALIST_NETS = 16
SEQUENCE_ITEMS = 4096
CAP = 64


def routing_tables(key):
    base = jax.random.fold_in(key, 4242)
    key_noise, key_hot, key_first, key_offset = jax.random.split(base, 4)
    blocks = SEQUENCE_ITEMS // TOK_DEV
    random_perturbation = jax.random.randint(key_noise, (SEQUENCE_ITEMS, SPECIALIST_NETS), 0, 65536, dtype=jnp.int32)
    hot_count = max(1, SPECIALIST_NETS // 16)
    favoured_specialists = jax.random.permutation(key_hot, SPECIALIST_NETS)[:hot_count]
    favoured_increment = jnp.zeros((SPECIALIST_NETS,), jnp.int32).at[favoured_specialists].set(16384)
    first_expert = jax.random.randint(key_first, (), 0, SPECIALIST_NETS, dtype=jnp.int32)
    offsets = jax.random.randint(key_offset, (blocks,), 0, TOK_DEV, dtype=jnp.int32)
    positions = jnp.arange(SEQUENCE_ITEMS, dtype=jnp.int32)
    within = jnp.mod(positions % TOK_DEV - offsets[positions // TOK_DEV], TOK_DEV)
    forced = within < 2 * CAP
    matrix_breadth = jnp.arange(SPECIALIST_NETS, dtype=jnp.int32)
    gating_scores = (random_perturbation + favoured_increment[None, :]) * SPECIALIST_NETS + matrix_breadth[None, :]
    gating_scores = gating_scores + jnp.where(forced[:, None] & (matrix_breadth[None, :] == first_expert), 1 << 30, 0).astype(jnp.int32)
    chosen = lax.top_k(gating_scores, TOP)[1].astype(jnp.int32)
    pairs = chosen.reshape(blocks, TOK_DEV * TOP)
    onehot = (pairs[:, :, None] == matrix_breadth[None, None, :]).astype(jnp.int32)
    rank_table = jnp.sum(jnp.cumsum(onehot, axis=1) * onehot, axis=2) - 1
    rank_table = rank_table.reshape(SEQUENCE_ITEMS, TOP)
    dropped_pairs = (rank_table >= CAP).astype(jnp.int32)
    slots = jnp.where(rank_table >= CAP, 0, rank_table).astype(jnp.int32)
    return (chosen, slots, dropped_pairs)


def draw_expert_ids(key, part):
    return routing_tables(key)[0]


def draw_slot_index(key, part):
    return routing_tables(key)[1]


def draw_dropped(key, part):
    return routing_tables(key)[2]


def block_scale(own_key, dims, shards, least, top_value):
    factor_of = 1.0
    for axis_at, shards_of in shards:
        steps = jax.random.uniform(jax.random.fold_in(jax.random.fold_in(own_key, 6), axis_at), (shards_of,), jnp.float32, least / len(shards), top_value / len(shards))
        factor_of = factor_of * jnp.repeat(jnp.exp(steps), dims[axis_at] // shards_of).reshape((-1,) + (1,) * (len(dims) - 1 - axis_at))
    return factor_of


def gaussian(stream_key, dims, spread, bound, cuts=(), kind=jnp.bfloat16):
    values = jax.random.normal(stream_key, dims, jnp.float32) * spread
    if len(cuts) > 0:
        values = block_scale(stream_key, dims, cuts, -0.22, 0.18) * values
    return jnp.clip(values, min=-bound, max=bound).astype(kind)


def setup_inputs(seed: int = 0) -> dict:
    streams_of = jax.random.split(jax.random.key(seed), 13)
    return {
        "tokens": gaussian(streams_of[0], (SEQUENCE_ITEMS, D), 1.0, 6.0, ((0, 32),)),
        "norm_gain": jnp.clip(1.0 + 0.18 * jax.random.normal(streams_of[1], (D,), jnp.float32), 0.1, 1.9),
        "expert_ids": draw_expert_ids(jax.random.fold_in(streams_of[12], 71), 0),
        "slot_index": draw_slot_index(jax.random.fold_in(streams_of[12], 71), 0),
        "dropped": draw_dropped(jax.random.fold_in(streams_of[12], 71), 0),
        "gates": jnp.clip(jnp.exp(math.log(0.8) - 2.7725887 * jax.random.uniform(streams_of[5], (SEQUENCE_ITEMS, TOP), jnp.float32) ** block_scale(streams_of[5], (SEQUENCE_ITEMS, TOP), ((0, 32),), -0.2, 0.2)), 0.05, 0.8),
        "w_gate": gaussian(streams_of[6], (SPECIALIST_NETS, D, FF), D ** -0.5, 0.125, ((0, 8), (2, 4))),
        "w_up": gaussian(streams_of[7], (SPECIALIST_NETS, D, FF), D ** -0.5, 0.125, ((0, 8), (2, 4))),
        "w_down": gaussian(streams_of[8], (SPECIALIST_NETS, D, FF), FF ** -0.5, 0.21875, ((0, 8), (2, 4))),
        "shared_gate": gaussian(streams_of[9], (D, SFF), D ** -0.5, 0.125, ((1, 4),)),
        "shared_up": gaussian(streams_of[10], (D, SFF), D ** -0.5, 0.125, ((1, 4),)),
        "shared_down": gaussian(streams_of[11], (SFF, D), SFF ** -0.5, 0.15625),
    }


norm_eps = 1e-06

def swiglu(left, right):
    return jax.nn.silu(left) * right

def reference(tokens, norm_gain, expert_ids, slot_index, dropped, gates, w_gate, w_up, w_down, shared_gate, shared_up, shared_down):
    values = tokens.astype(jnp.float32)
    scale = lax.rsqrt(lax.optimization_barrier(jnp.mean(values * values, axis=-1, keepdims=True)) + norm_eps)
    normed = (values * scale * norm_gain).astype(jnp.bfloat16)
    shared_gate_act = jnp.dot(normed, shared_gate, preferred_element_type=jnp.float32)
    shared_up_act = jnp.dot(normed, shared_up, preferred_element_type=jnp.float32)
    shared_hidden = swiglu(shared_gate_act, shared_up_act).astype(jnp.bfloat16)
    shared_out = jnp.dot(shared_hidden, shared_down, preferred_element_type=jnp.float32)
    blocks = SEQUENCE_ITEMS // TOK_DEV
    width = blocks * CAP
    token_index = jnp.broadcast_to(jnp.arange(SEQUENCE_ITEMS, dtype=jnp.int32)[:, None], (SEQUENCE_ITEMS, TOP))
    slot_row = expert_ids * width + token_index // TOK_DEV * CAP + slot_index
    slot_row = jnp.where(dropped == 0, slot_row, SPECIALIST_NETS * width).astype(jnp.int32)
    owner = jnp.full((SPECIALIST_NETS * width + 1,), SEQUENCE_ITEMS, jnp.int32)
    owner = owner.at[slot_row.reshape(-1)].set(token_index.reshape(-1).astype(jnp.int32))
    kept_gates = jnp.where(dropped == 0, gates, jnp.float32(0.0)).astype(jnp.float32)
    weight_table = jnp.zeros((SPECIALIST_NETS * width + 1,), jnp.float32).at[slot_row.reshape(-1)].set(kept_gates.reshape(-1))
    owner = owner[:-1].reshape(SPECIALIST_NETS, width)
    weight_table = weight_table[:-1].reshape(SPECIALIST_NETS, width)
    padded = jnp.concatenate([normed, jnp.zeros((1, D), jnp.bfloat16)], axis=0)

    def one_expert(running, inputs):
        picked, weights, gate_mat, up_mat, down_mat = inputs
        picked_rows = padded[picked].astype(jnp.float32)
        gate_act = jnp.dot(picked_rows, gate_mat.astype(jnp.float32), precision=lax.Precision.HIGHEST)
        up_act = jnp.dot(picked_rows, up_mat.astype(jnp.float32), precision=lax.Precision.HIGHEST)
        hidden = lax.optimization_barrier(swiglu(gate_act, up_act).astype(jnp.bfloat16)).astype(jnp.float32)
        expert_out = jnp.dot(hidden, down_mat.astype(jnp.float32).T, precision=lax.Precision.HIGHEST)
        expert_out = lax.optimization_barrier(expert_out.astype(jnp.bfloat16)).astype(jnp.float32)
        running = running.at[picked].add(weights[:, None] * expert_out)
        return (running, None)
    start = jnp.zeros((SEQUENCE_ITEMS + 1, D), jnp.float32)
    running, _ = lax.scan(one_expert, start, (owner, weight_table, w_gate, w_up, w_down))
    routed = running[:SEQUENCE_ITEMS]
    return (values + shared_out + routed).astype(jnp.bfloat16)
```

```python
import functools

import jax
import jax.numpy as jnp
from jax import lax
from jax.experimental import pallas as pl
from jax.experimental.pallas import tpu as pltpu
from jax.sharding import PartitionSpec as P

MESH = pl.DeviceIdType.MESH
CORES = 2
COLS = 2
VMEM_BYTES = 62 * 1024 * 1024
PIECES = 4

NT = (((1,), (1,)), ((), ()))
NN = (((1,), (0,)), ((), ()))


def dot(a, b, dims):
    return lax.dot_general(a, b, dims, preferred_element_type=jnp.float32)


def flip(index, mask, size):
    out, bit = 0, 1
    while bit < size:
        digit = (index // bit) % 2
        out = out + (1 - digit if mask & bit else digit) * bit
        bit *= 2
    return out


def layer_kernel(
    n_rows_z,
    tokens,
    gain,
    ids,
    dropped,
    gates,
    w_gate,
    w_up,
    w_down,
    s_gate,
    s_up,
    s_down,
    out,
    xb,
    wtb,
    gu,
    db,
    hb,
    sb,
    sg,
    su,
    sd,
    sh,
    whid,
    ysend,
    yrecv,
    ypart,
    zsend,
    zrecv,
    w_send,
    w_recv,
    own_sem,
    z_send,
    z_recv,
    y_send,
    y_recv,
    t_send,
    t_recv,
    h_send,
    h_recv,
    ry_send,
    ry_recv,
    rz_send,
    rz_recv,
):
    ep, tp = lax.axis_index("ep"), lax.axis_index("tp")
    z, y = ep // COLS, ep % COLS
    x, core = tp // CORES, tp % CORES
    rows, width = tokens.shape
    experts = w_gate.shape[0]
    hid = w_gate.shape[1]
    shid = s_gate.shape[0]
    piece = width // PIECES
    mate = (ep, x * CORES + 1 - core)
    across = (ep, (1 - x) * CORES + core)
    diagonal = (ep, (1 - x) * CORES + 1 - core)
    beside = (z * COLS + 1 - y, tp)
    along = [None] + [(flip(z, r, n_rows_z) * COLS + y, tp) for r in range(1, n_rows_z)]

    barrier = pltpu.get_barrier_semaphore()
    peers = [mate, across, diagonal, beside] + along[1:]
    for peer in peers:
        pl.semaphore_signal(barrier, inc=1, device_id=peer, device_id_type=MESH)

    def local(src, dst, sem):
        c = pltpu.make_async_copy(src, dst, sem)
        c.start()
        return c

    own = []
    chunks = []
    for e in range(experts):
        for m, source in enumerate((w_gate, w_up)):
            chunks.append((source.at[e], functools.partial(lambda e, m, s: gu.at[e, m, s], e, m)))
    first_down = len(chunks)
    for c in range(PIECES):
        cut = pl.ds(c * piece, piece)
        chunks.append(
            (w_down.at[:, :, cut], functools.partial(lambda cut, s: db.at[:, s, :, cut], cut))
        )
    for k, (source, place) in enumerate(chunks):
        own.append(local(source, place(0), own_sem.at[k]))
    n = len(chunks)
    shared_in = [local(s_gate, sg, own_sem.at[n]), local(s_up, su, own_sem.at[n + 1])]
    who = [tp, mate[1], across[1], diagonal[1]]
    shared_down_in = [
        local(
            s_down.at[pl.ds(pl.multiple_of(who[s] * shid, 16), shid), :],
            sd.at[s],
            own_sem.at[n + 2 + s],
        )
        for s in range(4)
    ]

    pl.semaphore_wait(barrier, len(peers))
    sent = []

    def remote(src, dst, ssem, rsem, peer):
        c = pltpu.make_async_remote_copy(
            src_ref=src,
            dst_ref=dst,
            send_sem=ssem,
            recv_sem=rsem,
            device_id=peer,
            device_id_type=MESH,
        )
        c.start()
        sent.append(c)
        return c

    far = [remote(s, p(2), w_send.at[1, k], w_recv.at[1, k], across) for k, (s, p) in enumerate(chunks)]
    near = [remote(s, p(1), w_send.at[0, k], w_recv.at[0, k], mate) for k, (s, p) in enumerate(chunks)]

    values = tokens[...].astype(jnp.float32)
    scale = lax.rsqrt(jnp.mean(values * values, axis=-1, keepdims=True) + 1e-06)
    xb[0, 0] = (values * scale * gain[...]).astype(jnp.bfloat16)
    table = jnp.zeros(wtb.shape[2:], jnp.float32)
    rows_of = lax.broadcasted_iota(jnp.int32, wtb.shape[2:], 0)
    for k in range(ids.shape[0]):
        hit = (ids[k : k + 1, :] == rows_of) & (dropped[k : k + 1, :] == 0)
        table = table + jnp.where(hit, gates[k : k + 1, :], 0.0)
    wtb[0, 0] = table

    rz, ry = [None], []
    for r in range(1, n_rows_z):
        rz.append(
            (
                remote(xb.at[0, 0], xb.at[0, r], z_send.at[0, r], z_recv.at[0, r], along[r]),
                remote(wtb.at[0, 0], wtb.at[0, r], z_send.at[1, r], z_recv.at[1, r], along[r]),
            )
        )

    def to_side(r):
        if r:
            for c in rz[r]:
                c.wait_recv()
        ry.append(
            (
                remote(xb.at[0, r], xb.at[1, r], y_send.at[0, r], y_recv.at[0, r], beside),
                remote(wtb.at[0, r], wtb.at[1, r], y_send.at[1, r], y_recv.at[1, r], beside),
            )
        )

    to_side(0)
    share_near = remote(xb.at[0, 0], sb.at[1], t_send.at[0], t_recv.at[0], mate)
    share_far = remote(xb.at[0, 0], sb.at[2], t_send.at[1], t_recv.at[1], across)

    passed = []

    def pass_on(k):
        far[k].wait_recv()
        place = chunks[k][1]
        passed.append(remote(place(2), place(3), w_send.at[2, k], w_recv.at[2, k], mate))

    def column(side, r, e):
        line = jnp.sum(
            jnp.where(rows_of == ep * experts + e, wtb[side, r], 0.0), axis=0, keepdims=True
        )
        return jnp.transpose(jnp.broadcast_to(line, (rows, rows)))[:, 0:1]

    def hidden(first, count, pair, e_first, e_count):
        def body(i, carry):
            e = e_first + i % e_count
            r = first + i // e_count
            left = jnp.concatenate([xb[0, r], xb[1, r]], axis=0)
            g = dot(left, gu[e, 0, 2 * pair : 2 * pair + 2].reshape(2 * hid, width), NT)
            u = dot(left, gu[e, 1, 2 * pair : 2 * pair + 2].reshape(2 * hid, width), NT)
            weight = jnp.concatenate([column(0, r, e), column(1, r, e)], axis=0)
            h = (g * jax.nn.sigmoid(g) * u * weight).astype(jnp.bfloat16)
            hb[0, e, pair, r] = h[:rows]
            hb[1, e, pair, r] = h[rows:]
            return carry

        lax.fori_loop(0, count * e_count, body, 0)

    def shared_hidden(pair):
        left = xb[0, 0] if pair == 0 else sb[2]
        left = jnp.concatenate([left, sb[2 * pair + 1]], axis=0)
        g = dot(left, sg[...], NT)
        u = dot(left, su[...], NT)
        h = (g * jax.nn.sigmoid(g) * u).astype(jnp.bfloat16)
        sh[2 * pair] = h[:rows]
        sh[2 * pair + 1] = h[rows:]

    for k in range(first_down):
        own[k].wait()
        near[k].wait_recv()
    to_side(1)
    for c in ry[0]:
        c.wait_recv()
    hidden(0, 1, 0, 0, experts)
    for c in shared_in:
        c.wait()
    share_near.wait_recv()
    shared_hidden(0)
    shs = [remote(sh.at[1], whid.at[1], h_send.at[0], h_recv.at[0], mate)]
    pass_on(0)
    for c in ry[1]:
        c.wait_recv()
    hidden(1, 1, 0, 0, experts)
    to_side(2)
    pass_on(1)
    passed[0].wait_recv()
    passed[1].wait_recv()
    hidden(0, 2, 1, 0, 1)
    for c in ry[2]:
        c.wait_recv()
    hidden(2, 1, 0, 0, experts)
    hidden(2, 1, 1, 0, 1)
    to_side(3)
    pass_on(2)
    for c in ry[3]:
        c.wait_recv()
    hidden(3, 1, 0, 0, experts)
    hidden(3, 1, 1, 0, 1)
    pass_on(3)
    passed[2].wait_recv()
    passed[3].wait_recv()
    hidden(0, n_rows_z, 1, 1, 1)

    ryd, rzd = [], []

    def down(c, side):
        cut = pl.ds(c * piece, piece)

        def body(q, carry):
            total = None
            for e in range(experts):
                for pair in range(2):
                    left = hb[side, e, pair, pl.ds(2 * q, 2)].reshape(2 * rows, 2 * hid)
                    right = db[e, 2 * pair : 2 * pair + 2, :, cut].reshape(2 * hid, piece)
                    part = dot(left, right, NN)
                    total = part if total is None else total + part
            total = total.reshape(2, rows, piece)
            if side:
                ysend[c, pl.ds(2 * q, 2)] = total.astype(jnp.bfloat16)
            else:
                ypart[c, pl.ds(2 * q, 2)] = total
            return carry

        lax.fori_loop(0, n_rows_z // 2, body, 0)

    def turn(c):
        ryd[c].wait_recv()
        for r in range(1, n_rows_z):
            both = ypart[c, r] + yrecv[c, r].astype(jnp.float32)
            zsend[c, r] = both.astype(jnp.bfloat16)
        rzd.append(
            [
                remote(zsend.at[c, r], zrecv.at[c, r], rz_send.at[c, r], rz_recv.at[c, r], along[r])
                for r in range(1, n_rows_z)
            ]
        )

    for c in range(PIECES):
        k = first_down + c
        own[k].wait()
        near[k].wait_recv()
        pass_on(k)
        passed[k].wait_recv()
        down(c, 1)
        ryd.append(remote(ysend.at[c], yrecv.at[c], ry_send.at[c], ry_recv.at[c], beside))
        down(c, 0)
        if c:
            turn(c - 1)

    share_far.wait_recv()
    share_on = remote(sb.at[2], sb.at[3], t_send.at[2], t_recv.at[2], mate)
    share_on.wait_recv()
    shared_hidden(1)
    shs.append(remote(sh.at[2], whid.at[2], h_send.at[1], h_recv.at[1], across))
    shs.append(remote(sh.at[3], whid.at[3], h_send.at[2], h_recv.at[2], diagonal))
    turn(PIECES - 1)
    for c in shared_down_in:
        c.wait()
    for c in shs:
        c.wait_recv()
    for c in range(PIECES):
        cut = pl.ds(c * piece, piece)
        total = tokens[:, cut].astype(jnp.float32) + dot(sh[0], sd[0, :, cut], NN)
        for s in range(1, 4):
            total = total + dot(whid[s], sd[s, :, cut], NN)
        total = total + (ypart[c, 0] + yrecv[c, 0].astype(jnp.float32))
        for r in range(1, n_rows_z):
            rzd[c][r - 1].wait_recv()
            total = total + zrecv[c, r].astype(jnp.float32)
        out[:, cut] = total.astype(out.dtype)
    for c in sent:
        c.wait_send()


def scratch_of(n_rows_z, rows, width, n_experts, experts, hid, shid):
    bf, f4 = jnp.bfloat16, jnp.float32
    piece = width // PIECES
    lines = n_experts
    pad = lambda v: -(-v // 128) * 128
    shapes = [
        ((COLS, n_rows_z, rows, width), bf),
        ((COLS, n_rows_z, lines, rows), f4),
        ((experts, 2, 4, hid, width), bf),
        ((experts, 4, hid, width), bf),
        ((COLS, experts, 2, n_rows_z, rows, 2 * hid), bf),
        ((4, rows, width), bf),
        ((shid, width), bf),
        ((shid, width), bf),
        ((4, shid, width), bf),
        ((4, rows, shid), bf),
        ((4, rows, shid), bf),
        ((PIECES, n_rows_z, rows, piece), bf),
        ((PIECES, n_rows_z, rows, piece), bf),
        ((PIECES, n_rows_z, rows, piece), f4),
        ((PIECES, n_rows_z, rows, piece), bf),
        ((PIECES, n_rows_z, rows, piece), bf),
    ]
    total = 0
    for dims, kind in shapes:
        size = pad(dims[-1]) * jnp.dtype(kind).itemsize
        for d in dims[:-1]:
            size *= d
        total += size
    n = 2 * experts + PIECES
    dma = pltpu.SemaphoreType.DMA
    sems = [dma((3, n)), dma((3, n)), dma((n + 6,))]
    sems += [dma((2, n_rows_z)) for _ in range(4)]
    sems += [dma((3,)) for _ in range(4)]
    sems += [dma((PIECES,)) for _ in range(2)]
    sems += [dma((PIECES, n_rows_z)) for _ in range(2)]
    return [pltpu.VMEM(d, k) for d, k in shapes] + sems, total


def fused(n_rows_z, scratch, tokens, gain, ids, slot, dropped, gates, wg, wu, wd, sg, su, sd):
    vmem = pl.BlockSpec(memory_space=pltpu.VMEM)
    hbm = pl.BlockSpec(memory_space=pl.ANY)
    return pl.pallas_call(
        functools.partial(layer_kernel, n_rows_z),
        out_shape=jax.ShapeDtypeStruct(tokens.shape, tokens.dtype),
        in_specs=[vmem] * 5 + [hbm] * 6,
        out_specs=vmem,
        scratch_shapes=scratch,
        compiler_params=pltpu.CompilerParams(
            collective_id=0, has_side_effects=True, vmem_limit_bytes=VMEM_BYTES
        ),
        name="moe_layer",
    )(
        tokens,
        gain[None, :],
        ids.T,
        dropped.T,
        gates.T,
        wg.transpose(0, 2, 1),
        wu.transpose(0, 2, 1),
        wd.transpose(0, 2, 1),
        sg.T,
        su.T,
        sd,
    )


TOP = 6
EXP_DEV = 2
TOK_DEV = 128


norm_eps = 1e-06


def swiglu(left, right):
    return jax.nn.silu(left) * right


def on_device(
    tokens,
    norm_gain,
    expert_ids,
    slot_index,
    dropped,
    gates,
    w_gate,
    w_up,
    w_down,
    shared_gate,
    shared_up,
    shared_down,
):
    n_expert_groups = lax.axis_size("ep")
    experts = EXP_DEV * n_expert_groups
    capacity = TOK_DEV * TOP * 4 // (experts * 3)
    model_width = tokens.shape[1]
    local_rows = tokens.shape[0]
    values = tokens.astype(jnp.float32)
    scale = lax.rsqrt(jnp.mean(values * values, axis=-1, keepdims=True) + norm_eps)
    normed = (values * scale * norm_gain).astype(jnp.bfloat16)
    destination_position = expert_ids * capacity + slot_index
    kept_pair = dropped == 0
    matrix_breadth = lax.iota(jnp.int32, experts * capacity)
    matches = (destination_position[:, :, None] == matrix_breadth[None, None, :]) & kept_pair[
        :, :, None
    ]
    dispatch_table = jnp.any(matches, axis=1).astype(jnp.bfloat16)
    outgoing = lax.dot_general(
        dispatch_table, normed, (((0,), (0,)), ((), ())), preferred_element_type=jnp.float32
    ).astype(jnp.bfloat16)
    boxes = outgoing.reshape(n_expert_groups, EXP_DEV, capacity, model_width)
    received = lax.all_to_all(boxes, "ep", split_axis=0, concat_axis=0, tiled=True)
    gate_all = lax.all_gather(w_gate, "tp", axis=2, tiled=True)
    up_all = lax.all_gather(w_up, "tp", axis=2, tiled=True)
    down_all = lax.all_gather(w_down, "tp", axis=2, tiled=True)
    gate_act = jnp.einsum("iecd,edf->iecf", received, gate_all, preferred_element_type=jnp.float32)
    up_act = jnp.einsum("iecd,edf->iecf", received, up_all, preferred_element_type=jnp.float32)
    hidden = swiglu(gate_act, up_act).astype(jnp.bfloat16)
    expert_out = jnp.einsum(
        "iecf,edf->iecd", hidden, down_all, preferred_element_type=jnp.float32
    ).astype(jnp.bfloat16)
    returned_output = lax.all_to_all(expert_out, "ep", split_axis=0, concat_axis=0, tiled=True)
    returned_rows = returned_output.reshape(experts * capacity, model_width)
    shard_piece = lax.all_gather(normed, "tp", axis=0, tiled=True)
    gate_act = jnp.dot(shard_piece, shared_gate, preferred_element_type=jnp.float32)
    up_act = jnp.dot(shard_piece, shared_up, preferred_element_type=jnp.float32)
    partial_hidden = swiglu(gate_act, up_act).astype(jnp.bfloat16)
    whole_hidden = lax.all_to_all(partial_hidden, "tp", split_axis=0, concat_axis=1, tiled=True)
    shared_out = jnp.dot(whole_hidden, shared_down, preferred_element_type=jnp.float32)
    safe_target = jnp.where(kept_pair, destination_position, 0)
    picked = jnp.take(returned_rows, safe_target.reshape(-1), axis=0).reshape(
        local_rows, TOP, model_width
    )
    kept_weights = jnp.where(kept_pair, gates, jnp.float32(0.0))
    routed = jnp.sum(picked.astype(jnp.float32) * kept_weights[:, :, None], axis=1)
    return (values + shared_out + routed).astype(jnp.bfloat16)


def solution(mesh):
    ep, tp = mesh.shape["ep"], mesh.shape["tp"]
    placed = (
        P(("ep", "tp"), None),
        P(),
        P(("ep", "tp"), None),
        P(("ep", "tp"), None),
        P(("ep", "tp"), None),
        P(("ep", "tp"), None),
        P("ep", None, "tp"),
        P("ep", None, "tp"),
        P("ep", None, "tp"),
        P(None, "tp"),
        P(None, "tp"),
        P(),
    )

    def layer(*args):
        tokens, w_gate, shared_gate = args[0], args[6], args[9]
        n_rows_z = ep // COLS
        scratch, size = scratch_of(
            n_rows_z,
            tokens.shape[0],
            tokens.shape[1],
            ep * w_gate.shape[0],
            w_gate.shape[0],
            w_gate.shape[2],
            shared_gate.shape[1],
        )
        spare = 8 * 1024 * 1024
        if tp == 2 * CORES and n_rows_z == 4 and size + spare < VMEM_BYTES:
            return fused(n_rows_z, scratch, *args)
        return on_device(*args)

    return jax.shard_map(
        layer, mesh=mesh, in_specs=placed, out_specs=P(("ep", "tp"), None), check_vma=False
    )
```

```python
import functools

import jax
import jax.numpy as jnp
from jax import lax
from jax.experimental import pallas as pl
from jax.experimental.pallas import tpu as pltpu
from jax.sharding import PartitionSpec as P

MESH = pl.DeviceIdType.MESH
CORES = 2
COLS = 2
VMEM_BYTES = 62 * 1024 * 1024
PIECES = 8

NT = (((1,), (1,)), ((), ()))
NN = (((1,), (0,)), ((), ()))


def dot(a, b, dims):
    return lax.dot_general(a, b, dims, preferred_element_type=jnp.float32)


def flip(index, mask, size):
    out, bit = 0, 1
    while bit < size:
        digit = (index // bit) % 2
        out = out + (1 - digit if mask & bit else digit) * bit
        bit *= 2
    return out


def layer_kernel(
    n_rows_z,
    tokens,
    gain,
    ids,
    dropped,
    gates,
    w_gate,
    w_up,
    w_down,
    s_gate,
    s_up,
    s_down,
    out,
    xb,
    wtb,
    gu,
    ga,
    db,
    hb,
    sb,
    sg,
    su,
    sd,
    sh,
    whid,
    ysend,
    yrecv,
    ypart,
    zsend,
    zrecv,
    w_send,
    w_recv,
    own_sem,
    z_send,
    z_recv,
    y_send,
    y_recv,
    t_send,
    t_recv,
    h_send,
    h_recv,
    ry_send,
    ry_recv,
    rz_send,
    rz_recv,
):
    ep, tp = lax.axis_index("ep"), lax.axis_index("tp")
    z, y = ep // COLS, ep % COLS
    x, core = tp // CORES, tp % CORES
    rows, width = tokens.shape
    experts = w_gate.shape[0]
    hid = w_gate.shape[1]
    shid = s_gate.shape[0]
    piece = width // PIECES
    mate = (ep, x * CORES + 1 - core)
    across = (ep, (1 - x) * CORES + core)
    diagonal = (ep, (1 - x) * CORES + 1 - core)
    beside = (z * COLS + 1 - y, tp)
    along = [None] + [(flip(z, r, n_rows_z) * COLS + y, tp) for r in range(1, n_rows_z)]

    barrier = pltpu.get_barrier_semaphore()
    peers = [mate, across, diagonal, beside] + along[1:]
    for peer in peers:
        pl.semaphore_signal(barrier, inc=1, device_id=peer, device_id_type=MESH)

    def local(src, dst, sem):
        c = pltpu.make_async_copy(src, dst, sem)
        c.start()
        return c

    own = []
    chunks = []
    for e in range(experts):
        for m, source in enumerate((w_gate, w_up)):
            chunks.append((source.at[e], functools.partial(lambda e, m, s: gu.at[e, m, s], e, m)))
    first_down = len(chunks)
    for c in range(PIECES):
        cut = pl.ds(c * piece, piece)
        chunks.append(
            (w_down.at[:, :, cut], functools.partial(lambda cut, s: db.at[:, s, :, cut], cut))
        )
    for k, (source, place) in enumerate(chunks):
        own.append(local(source, place(0), own_sem.at[k]))
    n = len(chunks)
    shared_in = [local(s_gate, sg, own_sem.at[n]), local(s_up, su, own_sem.at[n + 1])]
    who = [tp, mate[1], across[1], diagonal[1]]
    shared_down_in = [
        local(
            s_down.at[pl.ds(pl.multiple_of(who[s] * shid, 16), shid), :],
            sd.at[s],
            own_sem.at[n + 2 + s],
        )
        for s in range(4)
    ]

    pl.semaphore_wait(barrier, len(peers))
    sent = []

    def remote(src, dst, ssem, rsem, peer):
        c = pltpu.make_async_remote_copy(
            src_ref=src,
            dst_ref=dst,
            send_sem=ssem,
            recv_sem=rsem,
            device_id=peer,
            device_id_type=MESH,
        )
        c.start()
        sent.append(c)
        return c

    early = first_down + PIECES // 2

    def send_far(first, last):
        for k in range(first, last):
            source, place = chunks[k]
            far.append(remote(source, place(2), w_send.at[1, k], w_recv.at[1, k], across))

    far = []
    send_far(0, early)
    near = [remote(s, p(1), w_send.at[0, k], w_recv.at[0, k], mate) for k, (s, p) in enumerate(chunks)]

    values = tokens[...].astype(jnp.float32)
    scale = lax.rsqrt(jnp.mean(values * values, axis=-1, keepdims=True) + 1e-06)
    xb[0, 0] = (values * scale * gain[...]).astype(jnp.bfloat16)
    table = jnp.zeros(wtb.shape[2:], jnp.float32)
    rows_of = lax.broadcasted_iota(jnp.int32, wtb.shape[2:], 0)
    for k in range(ids.shape[0]):
        hit = (ids[k : k + 1, :] == rows_of) & (dropped[k : k + 1, :] == 0)
        table = table + jnp.where(hit, gates[k : k + 1, :], 0.0)
    wtb[0, 0] = table

    half = rows // 2
    parts = [(wtb, ())] + [(xb, (pl.ds(i * half, half),)) for i in range(2)]

    def part_of(i, side, r):
        ref, cut = parts[i]
        return ref.at[(side, r) + cut]

    rz, ry = [None], []
    for r in range(1, n_rows_z):
        rz.append(
            [
                remote(
                    part_of(i, 0, 0), part_of(i, 0, r), z_send.at[i, r], z_recv.at[i, r], along[r]
                )
                for i in range(3)
            ]
        )

    def to_side(r):
        ry.append([])
        for i in range(3):
            if r:
                rz[r][i].wait_recv()
            ry[r].append(
                remote(
                    part_of(i, 0, r), part_of(i, 1, r), y_send.at[i, r], y_recv.at[i, r], beside
                )
            )

    to_side(0)
    share_near = remote(xb.at[0, 0], sb.at[1], t_send.at[0], t_recv.at[0], mate)
    share_far = remote(xb.at[0, 0], sb.at[2], t_send.at[1], t_recv.at[1], across)
    send_far(early, n)

    passed = []

    def pass_on(k):
        far[k].wait_recv()
        place = chunks[k][1]
        passed.append(remote(place(2), place(3), w_send.at[2, k], w_recv.at[2, k], mate))

    def column(side, r, e):
        line = jnp.sum(
            jnp.where(rows_of == ep * experts + e, wtb[side, r], 0.0), axis=0, keepdims=True
        )
        return jnp.transpose(jnp.broadcast_to(line, (rows, rows)))[:, 0:1]

    def gate_only(first, count, e):
        def body(r, carry):
            left = jnp.concatenate([xb[0, r], xb[1, r]], axis=0)
            ga[r] = dot(left, gu[e, 0, 2:4].reshape(2 * hid, width), NT)
            return carry

        lax.fori_loop(first, first + count, body, 0)

    def hidden(first, count, pair, e_first, e_count, stored=False):
        def body(i, carry):
            e = e_first + i % e_count
            r = first + i // e_count
            left = jnp.concatenate([xb[0, r], xb[1, r]], axis=0)
            if stored:
                g = ga[r]
            else:
                g = dot(left, gu[e, 0, 2 * pair : 2 * pair + 2].reshape(2 * hid, width), NT)
            u = dot(left, gu[e, 1, 2 * pair : 2 * pair + 2].reshape(2 * hid, width), NT)
            weight = jnp.concatenate([column(0, r, e), column(1, r, e)], axis=0)
            h = (g * jax.nn.sigmoid(g) * u * weight).astype(jnp.bfloat16)
            hb[0, e, pair, r] = h[:rows]
            hb[1, e, pair, r] = h[rows:]
            return carry

        lax.fori_loop(0, count * e_count, body, 0)

    def shared_hidden(pair):
        left = xb[0, 0] if pair == 0 else sb[2]
        left = jnp.concatenate([left, sb[2 * pair + 1]], axis=0)
        g = dot(left, sg[...], NT)
        u = dot(left, su[...], NT)
        h = (g * jax.nn.sigmoid(g) * u).astype(jnp.bfloat16)
        sh[2 * pair] = h[:rows]
        sh[2 * pair + 1] = h[rows:]

    for k in range(first_down):
        own[k].wait()
        near[k].wait_recv()
    to_side(1)
    for c in ry[0]:
        c.wait_recv()
    hidden(0, 1, 0, 0, experts)
    for c in shared_in:
        c.wait()
    share_near.wait_recv()
    shared_hidden(0)
    shs = [remote(sh.at[1], whid.at[1], h_send.at[0], h_recv.at[0], mate)]
    pass_on(0)
    for c in ry[1]:
        c.wait_recv()
    hidden(1, 1, 0, 0, experts)
    to_side(2)
    pass_on(1)
    passed[0].wait_recv()
    passed[1].wait_recv()
    hidden(0, 2, 1, 0, 1)
    for c in ry[2]:
        c.wait_recv()
    hidden(2, 1, 0, 0, experts)
    hidden(2, 1, 1, 0, 1)
    to_side(3)
    pass_on(2)
    passed[2].wait_recv()
    gate_only(0, 3, 1)
    for c in ry[3]:
        c.wait_recv()
    hidden(3, 1, 0, 0, experts)
    hidden(3, 1, 1, 0, 1)
    gate_only(3, 1, 1)
    pass_on(3)
    passed[3].wait_recv()
    hidden(0, n_rows_z, 1, 1, 1, stored=True)

    ryd, rzd = [], []

    def down(c, side):
        cut = pl.ds(c * piece, piece)

        def body(q, carry):
            total = None
            for e in range(experts):
                for pair in range(2):
                    left = hb[side, e, pair, pl.ds(2 * q, 2)].reshape(2 * rows, 2 * hid)
                    right = db[e, 2 * pair : 2 * pair + 2, :, cut].reshape(2 * hid, piece)
                    part = dot(left, right, NN)
                    total = part if total is None else total + part
            total = total.reshape(2, rows, piece)
            if side:
                ysend[c, pl.ds(2 * q, 2)] = total.astype(jnp.bfloat16)
            else:
                ypart[c, pl.ds(2 * q, 2)] = total
            return carry

        lax.fori_loop(0, n_rows_z // 2, body, 0)

    def turn(c):
        ryd[c].wait_recv()
        for r in range(1, n_rows_z):
            both = ypart[c, r] + yrecv[c, r].astype(jnp.float32)
            zsend[c, r] = both.astype(jnp.bfloat16)
        rzd.append(
            [
                remote(zsend.at[c, r], zrecv.at[c, r], rz_send.at[c, r], rz_recv.at[c, r], along[r])
                for r in range(1, n_rows_z)
            ]
        )

    for c in range(PIECES):
        k = first_down + c
        own[k].wait()
        near[k].wait_recv()
        pass_on(k)
        passed[k].wait_recv()
        down(c, 1)
        ryd.append(remote(ysend.at[c], yrecv.at[c], ry_send.at[c], ry_recv.at[c], beside))
        down(c, 0)
        if c:
            turn(c - 1)
        if c == PIECES - 3:
            share_far.wait_recv()
            share_on = remote(sb.at[2], sb.at[3], t_send.at[2], t_recv.at[2], mate)
            share_on.wait_recv()
            shared_hidden(1)
            shs.append(remote(sh.at[2], whid.at[2], h_send.at[1], h_recv.at[1], across))
            shs.append(remote(sh.at[3], whid.at[3], h_send.at[2], h_recv.at[2], diagonal))

    for c in shared_down_in:
        c.wait()
    for c in shs:
        c.wait_recv()

    def base(c, carry):
        cut = pl.ds(pl.multiple_of(c * piece, piece), piece)
        total = tokens[:, cut].astype(jnp.float32) + dot(sh[0], sd[0, :, cut], NN)
        for s in range(1, 4):
            total = total + dot(whid[s], sd[s, :, cut], NN)
        ypart[c, 0] = ypart[c, 0] + total
        return carry

    lax.fori_loop(0, PIECES, base, 0)
    turn(PIECES - 1)
    for c in range(PIECES):
        cut = pl.ds(c * piece, piece)
        total = ypart[c, 0] + yrecv[c, 0].astype(jnp.float32)
        for r in range(1, n_rows_z):
            rzd[c][r - 1].wait_recv()
            total = total + zrecv[c, r].astype(jnp.float32)
        out[:, cut] = total.astype(out.dtype)
    for c in sent:
        c.wait_send()


def scratch_of(n_rows_z, rows, width, n_experts, experts, hid, shid):
    bf, f4 = jnp.bfloat16, jnp.float32
    piece = width // PIECES
    lines = n_experts
    pad = lambda v: -(-v // 128) * 128
    shapes = [
        ((COLS, n_rows_z, rows, width), bf),
        ((COLS, n_rows_z, lines, rows), f4),
        ((experts, 2, 4, hid, width), bf),
        ((n_rows_z, 2 * rows, 2 * hid), f4),
        ((experts, 4, hid, width), bf),
        ((COLS, experts, 2, n_rows_z, rows, 2 * hid), bf),
        ((4, rows, width), bf),
        ((shid, width), bf),
        ((shid, width), bf),
        ((4, shid, width), bf),
        ((4, rows, shid), bf),
        ((4, rows, shid), bf),
        ((PIECES, n_rows_z, rows, piece), bf),
        ((PIECES, n_rows_z, rows, piece), bf),
        ((PIECES, n_rows_z, rows, piece), f4),
        ((PIECES, n_rows_z, rows, piece), bf),
        ((PIECES, n_rows_z, rows, piece), bf),
    ]
    total = 0
    for dims, kind in shapes:
        size = pad(dims[-1]) * jnp.dtype(kind).itemsize
        for d in dims[:-1]:
            size *= d
        total += size
    n = 2 * experts + PIECES
    dma = pltpu.SemaphoreType.DMA
    sems = [dma((3, n)), dma((3, n)), dma((n + 6,))]
    sems += [dma((3, n_rows_z)) for _ in range(4)]
    sems += [dma((3,)) for _ in range(4)]
    sems += [dma((PIECES,)) for _ in range(2)]
    sems += [dma((PIECES, n_rows_z)) for _ in range(2)]
    return [pltpu.VMEM(d, k) for d, k in shapes] + sems, total


def fused(n_rows_z, scratch, tokens, gain, ids, slot, dropped, gates, wg, wu, wd, sg, su, sd):
    vmem = pl.BlockSpec(memory_space=pltpu.VMEM)
    hbm = pl.BlockSpec(memory_space=pl.ANY)
    return pl.pallas_call(
        functools.partial(layer_kernel, n_rows_z),
        out_shape=jax.ShapeDtypeStruct(tokens.shape, tokens.dtype),
        in_specs=[vmem] * 5 + [hbm] * 6,
        out_specs=vmem,
        scratch_shapes=scratch,
        compiler_params=pltpu.CompilerParams(
            collective_id=0, has_side_effects=True, vmem_limit_bytes=VMEM_BYTES
        ),
        name="moe_layer",
    )(
        tokens,
        gain[None, :],
        ids.T,
        dropped.T,
        gates.T,
        wg.transpose(0, 2, 1),
        wu.transpose(0, 2, 1),
        wd.transpose(0, 2, 1),
        sg.T,
        su.T,
        sd,
    )


TOP = 6
EXP_DEV = 2
TOK_DEV = 128


norm_eps = 1e-06


def swiglu(left, right):
    return jax.nn.silu(left) * right


def on_device(
    tokens,
    norm_gain,
    expert_ids,
    slot_index,
    dropped,
    gates,
    w_gate,
    w_up,
    w_down,
    shared_gate,
    shared_up,
    shared_down,
):
    n_expert_groups = lax.axis_size("ep")
    experts = EXP_DEV * n_expert_groups
    capacity = TOK_DEV * TOP * 4 // (experts * 3)
    model_width = tokens.shape[1]
    local_rows = tokens.shape[0]
    values = tokens.astype(jnp.float32)
    scale = lax.rsqrt(jnp.mean(values * values, axis=-1, keepdims=True) + norm_eps)
    normed = (values * scale * norm_gain).astype(jnp.bfloat16)
    destination_position = expert_ids * capacity + slot_index
    kept_pair = dropped == 0
    matrix_breadth = lax.iota(jnp.int32, experts * capacity)
    matches = (destination_position[:, :, None] == matrix_breadth[None, None, :]) & kept_pair[
        :, :, None
    ]
    dispatch_table = jnp.any(matches, axis=1).astype(jnp.bfloat16)
    outgoing = lax.dot_general(
        dispatch_table, normed, (((0,), (0,)), ((), ())), preferred_element_type=jnp.float32
    ).astype(jnp.bfloat16)
    boxes = outgoing.reshape(n_expert_groups, EXP_DEV, capacity, model_width)
    received = lax.all_to_all(boxes, "ep", split_axis=0, concat_axis=0, tiled=True)
    gate_all = lax.all_gather(w_gate, "tp", axis=2, tiled=True)
    up_all = lax.all_gather(w_up, "tp", axis=2, tiled=True)
    down_all = lax.all_gather(w_down, "tp", axis=2, tiled=True)
    gate_act = jnp.einsum("iecd,edf->iecf", received, gate_all, preferred_element_type=jnp.float32)
    up_act = jnp.einsum("iecd,edf->iecf", received, up_all, preferred_element_type=jnp.float32)
    hidden = swiglu(gate_act, up_act).astype(jnp.bfloat16)
    expert_out = jnp.einsum(
        "iecf,edf->iecd", hidden, down_all, preferred_element_type=jnp.float32
    ).astype(jnp.bfloat16)
    returned_output = lax.all_to_all(expert_out, "ep", split_axis=0, concat_axis=0, tiled=True)
    returned_rows = returned_output.reshape(experts * capacity, model_width)
    shard_piece = lax.all_gather(normed, "tp", axis=0, tiled=True)
    gate_act = jnp.dot(shard_piece, shared_gate, preferred_element_type=jnp.float32)
    up_act = jnp.dot(shard_piece, shared_up, preferred_element_type=jnp.float32)
    partial_hidden = swiglu(gate_act, up_act).astype(jnp.bfloat16)
    whole_hidden = lax.all_to_all(partial_hidden, "tp", split_axis=0, concat_axis=1, tiled=True)
    shared_out = jnp.dot(whole_hidden, shared_down, preferred_element_type=jnp.float32)
    safe_target = jnp.where(kept_pair, destination_position, 0)
    picked = jnp.take(returned_rows, safe_target.reshape(-1), axis=0).reshape(
        local_rows, TOP, model_width
    )
    kept_weights = jnp.where(kept_pair, gates, jnp.float32(0.0))
    routed = jnp.sum(picked.astype(jnp.float32) * kept_weights[:, :, None], axis=1)
    return (values + shared_out + routed).astype(jnp.bfloat16)


def solution(mesh):
    ep, tp = mesh.shape["ep"], mesh.shape["tp"]
    placed = (
        P(("ep", "tp"), None),
        P(),
        P(("ep", "tp"), None),
        P(("ep", "tp"), None),
        P(("ep", "tp"), None),
        P(("ep", "tp"), None),
        P("ep", None, "tp"),
        P("ep", None, "tp"),
        P("ep", None, "tp"),
        P(None, "tp"),
        P(None, "tp"),
        P(),
    )

    def layer(*args):
        tokens, w_gate, shared_gate = args[0], args[6], args[9]
        n_rows_z = ep // COLS
        scratch, size = scratch_of(
            n_rows_z,
            tokens.shape[0],
            tokens.shape[1],
            ep * w_gate.shape[0],
            w_gate.shape[0],
            w_gate.shape[2],
            shared_gate.shape[1],
        )
        spare = 8 * 1024 * 1024
        if tp == 2 * CORES and n_rows_z == 4 and w_gate.shape[0] == 2 and size + spare < VMEM_BYTES:
            return fused(n_rows_z, scratch, *args)
        return on_device(*args)

    return jax.shard_map(
        layer, mesh=mesh, in_specs=placed, out_specs=P(("ep", "tp"), None), check_vma=False
    )
```
